32 devices in a mesh: dp: 8 (over y, x, core), tensor: 4 (over z).
Axes of the slice: x: 2, y: 2, z: 4, core: 2. Of those that a mesh axis runs over, the one named last changes fastest.
Arguments:
- tokens: bfloat16 [512, 8192], P('dp'), may hold values from -6 to 6
- gate_weight: bfloat16 [8192, 14848], P('dp', 'tensor'), may hold values from -0.09375 to 0.09375
- up_weight: bfloat16 [8192, 14848], P('dp', 'tensor'), may hold values from -0.09375 to 0.09375
- down_weight: bfloat16 [14848, 8192], P('tensor', 'dp'), may hold values from -6 to 6
- channel_group: int32 [14848], P('tensor'), may hold values from 0 to 115, as said below
- owners: int32 [116], replicated, may hold values from 0 to 3
Outputs:
- group_scores: float32 [4, 116], P('tensor')
The draws below stay inside these ranges and needn't reach their ends.
Inputs may be any that keep to these rules, and one draw needn't show every extreme that they name: `channel_group`: every group 0 to 115 has exactly 128 channels.
All inputs are finite; a program needn't handle non-finite values.
Results may differ from the reference program's by a relative error of at most 0.0044.
Values may be sent and summed in bfloat16 or wider, within the bound.
No kernel may reach another device: no remote copies, remote signals or barrier semaphores. Data moves between devices by JAX's collectives and lax.ppermute only.
A program may use at most 128 MiB of HBM per device.

```python
import jax
import jax.numpy as jnp
from jax import lax

D = 8192
FF = 14848
GROUP = 128
TOKENS = 512
GROUPS = 116
N_DP = 8
N_TENSOR = 4


def draw_channel_group(key, part):
    order = jax.random.permutation(jax.random.fold_in(key, 7), FF)
    return (order // GROUP).astype(jnp.int32)


def with_ends(result, own_key, low, high):
    extent = result.shape
    index_at = [jax.random.randint(jax.random.fold_in(own_key, axis), (), 0, extent[axis]) for axis in range(len(extent))]
    result = result.at[tuple(index_at)].set(low)
    longest = extent.index(max(extent))
    index_at[longest] = (index_at[longest] + 1) % extent[longest]
    return result.at[tuple(index_at)].set(high)


def spiked(drawn, own_key, source, target, blocks, factor):
    def block_of(position):
        return (jnp.arange(drawn.shape[position]) // (drawn.shape[position] // blocks)).reshape((-1,) + (1,) * (drawn.ndim - 1 - position))

    near = jax.random.permutation(own_key, blocks)[block_of(target)]
    second = (block_of(target) + blocks // 2) % blocks
    return jnp.where((block_of(source) == near) | (block_of(source) == second), factor * drawn, drawn)


def block_scale(stream_key, extent, shards, low, largest):
    level, own = 1.0, jax.random.fold_in(stream_key, 6)
    for position, blocks in shards:
        draws = jnp.exp(jax.random.uniform(jax.random.fold_in(own, position), (blocks,), jnp.float32, low / len(shards), largest / len(shards)))
        level = level * jnp.repeat(draws, extent[position] // blocks).reshape([-1 if axis == position else 1 for axis in range(len(extent))])
    return level


def noise(own_key, extent, spread, most, split=(), kind=jnp.bfloat16):
    result = jax.random.normal(own_key, extent, jnp.float32) * spread
    if len(split) > 0:
        result = block_scale(own_key, extent, split, -0.22, 0.18) * result
    return jnp.clip(result, min=-most, max=most).astype(kind)


def heavy_noise(stream_key, shape, spread, bound, cuts, heavy, held_as=jnp.bfloat16):
    entries = spread * jax.random.normal(stream_key, shape, jnp.float32)
    if cuts:
        entries = entries * block_scale(stream_key, shape, cuts, -0.22, 0.18)
    return jnp.clip(spiked(entries, jax.random.fold_in(stream_key, 3), *heavy), -bound, bound).astype(held_as)


def setup_inputs(seed: int = 0) -> dict:
    key_of = jax.random.split(jax.random.key(seed), 7)
    return {
        "tokens": noise(key_of[0], (TOKENS, D), 1.0, 6.0, ((0, 8),)),
        "gate_weight": heavy_noise(key_of[1], (D, FF), D ** -0.5, 0.09375, ((0, 8), (1, 4)), (0, 1, 8, 2.0)),
        "up_weight": heavy_noise(key_of[2], (D, FF), D ** -0.5, 0.09375, ((0, 8), (1, 4)), (0, 1, 8, 2.0)),
        "down_weight": heavy_noise(key_of[3], (FF, D), 1.0, 6.0, ((0, 4), (1, 8)), (1, 0, 8, 2.0)),
        "channel_group": draw_channel_group(jax.random.fold_in(key_of[6], 71), 0),
        "owners": with_ends(jax.random.randint(key_of[5], (GROUPS,), 0, N_TENSOR), jax.random.fold_in(key_of[5], 1), 0, N_TENSOR - 1).astype(jnp.int32),
    }


def reference(tokens, gate_weight, up_weight, down_weight, channel_group, owners):
    block = D // N_DP
    x_blocks = tokens.reshape(TOKENS, N_DP, block).transpose(1, 0, 2)
    g_blocks = gate_weight.reshape(N_DP, block, FF)
    u_blocks = up_weight.reshape(N_DP, block, FF)

    def add_block(carry, item):
        x_part, g_part, u_part = item
        pg = jnp.dot(x_part, g_part, preferred_element_type=jnp.float32).astype(jnp.bfloat16)
        pu = jnp.dot(x_part, u_part, preferred_element_type=jnp.float32).astype(jnp.bfloat16)
        pg, pu = lax.optimization_barrier((pg, pu))
        return ((carry[0] + pg.astype(jnp.float32), carry[1] + pu.astype(jnp.float32)), None)
    start = jnp.zeros((TOKENS, FF), jnp.float32)
    (gate, up), _ = lax.scan(add_block, (start, start), (x_blocks, g_blocks, u_blocks))
    hidden = jax.nn.silu(gate) * up
    energy = lax.optimization_barrier(jnp.sum(hidden * hidden, axis=0)) / TOKENS
    magnitude = lax.optimization_barrier(jnp.sum(jnp.abs(down_weight.astype(jnp.float32)), axis=1)) / D
    channel_score = jnp.sqrt(energy) * magnitude
    onehot = (channel_group[:, None] == jnp.arange(GROUPS, dtype=jnp.int32)[None, :]).astype(jnp.float32)
    totals = jnp.dot(channel_score, onehot, precision=lax.Precision.HIGHEST) / GROUP
    ranks = jnp.arange(N_TENSOR, dtype=jnp.int32)[:, None]
    return jnp.where(owners[None, :] == ranks, totals[None, :], jnp.float32(0.0))
```

```python
import jax
import jax.numpy as jnp
from jax import lax
from jax.experimental import pallas as pl
from jax.experimental.pallas import tpu as pltpu
from jax.sharding import PartitionSpec as P

GROUP = 128
CHUNKS = 2
COLUMNS = 256


def swap(value, axis, mask):
    size = lax.axis_size(axis)
    return lax.ppermute(value, axis, [(i, i ^ mask) for i in range(size)])


def total(value, axis, groups):
    for bits in groups:
        masks = [0]
        for bit in bits:
            masks += [m ^ (1 << bit) for m in masks]
        value = sum([swap(value, axis, m) for m in masks[1:]], value)
    return value


def group_bits(first, count):
    groups = [[b] for b in range(min(first, count))]
    rest = list(range(first, count))
    return groups + [rest[i : i + 2] for i in range(0, len(rest), 2)]


def block_order(bits):
    length = len(bits)
    return [sum(((p >> (length - 1 - i)) & 1) << b for i, b in enumerate(bits)) for p in range(1 << length)]


def product(blocks, weight, chunk, chunks):
    count = len(blocks)
    rows = blocks[0].shape[0] // chunks
    depth, width = weight.shape
    half = count // 2 * rows

    def kernel(*refs):
        xs, w, keep, send, lhs = refs[:count], refs[count], refs[count + 1], refs[count + 2], refs[count + 3]

        @pl.when(pl.program_id(0) == 0)
        def _():
            for i, x in enumerate(xs):
                lhs[i * rows : (i + 1) * rows, :] = x[...]

        part = jnp.dot(lhs[...], w[...], preferred_element_type=jnp.float32).astype(jnp.bfloat16)
        keep[...] = part[:half]
        send[...] = part[half:]

    out = jax.ShapeDtypeStruct((half, width), jnp.bfloat16)
    return pl.pallas_call(
        kernel,
        out_shape=(out, out),
        grid=(pl.cdiv(width, COLUMNS),),
        in_specs=[pl.BlockSpec((rows, depth), lambda j: (chunk, 0))] * count
        + [pl.BlockSpec((depth, COLUMNS), lambda j: (0, j))],
        out_specs=(pl.BlockSpec((half, COLUMNS), lambda j: (0, j)),) * 2,
        scratch_shapes=[pltpu.VMEM((count * rows, depth), jnp.bfloat16)],
        cost_estimate=pl.CostEstimate(
            flops=2 * count * rows * depth * width, transcendentals=0, bytes_accessed=2 * depth * width
        ),
    )(*blocks, weight)


def add(a, b):
    return a.astype(jnp.float32) + b.astype(jnp.float32)


def scatter_sum(keep, send, bits):
    for step, bit in enumerate(bits):
        got = swap(send, "dp", 1 << bit)
        if step == len(bits) - 1:
            return add(keep, got)
        half = keep.shape[0] // 2
        send = add(keep[half:], got[half:]).astype(jnp.bfloat16)
        keep = add(keep[:half], got[:half]).astype(jnp.bfloat16)


def shards(tokens, gate_weight, up_weight, down_weight, channel_group, owners):
    size = lax.axis_size("dp")
    levels = size.bit_length() - 1
    tensor_levels = lax.axis_size("tensor").bit_length() - 1
    me = lax.axis_index("dp")
    total_tokens = tokens.shape[0] * size
    model_width = tokens.shape[1]
    block = gate_weight.shape[0]
    group_count = owners.shape[0]
    blocks = [lax.dynamic_slice_in_dim(tokens, (me ^ k) * block, block, axis=1) for k in range(size)]
    blocks = [b if k == 0 else swap(b, "dp", k) for k, b in enumerate(blocks)]
    magnitude = jnp.sum(jnp.abs(down_weight.astype(jnp.float32)), axis=1) / model_width
    magnitude = total(magnitude, "dp", group_bits(1, levels))
    gate_bits = list(range(levels))
    up_bits = gate_bits[:1] + gate_bits[:0:-1]
    energy = 0.0
    for chunk in range(CHUNKS):
        gate = scatter_sum(*product([blocks[k] for k in block_order(gate_bits)], gate_weight, chunk, CHUNKS), gate_bits)
        up = scatter_sum(*product([blocks[k] for k in block_order(up_bits)], up_weight, chunk, CHUNKS), up_bits)
        hidden = jax.nn.silu(gate) * up
        energy += jnp.sum(hidden * hidden, axis=0)
    energy = total(energy / total_tokens, "dp", group_bits(1, levels))
    onehot = (channel_group[:, None] == jnp.arange(group_count, dtype=jnp.int32)[None, :]).astype(jnp.float32)
    totals = jnp.dot(jnp.sqrt(energy) * magnitude, onehot, precision=lax.Precision.HIGHEST) / GROUP
    totals = total(totals, "tensor", group_bits(0, tensor_levels))
    row = jnp.where(owners == lax.axis_index("tensor"), totals, jnp.float32(0.0))
    return row[None, :]


def solution(mesh):
    return jax.shard_map(
        shards,
        mesh=mesh,
        in_specs=(P("dp", None), P("dp", "tensor"), P("dp", "tensor"), P("tensor", "dp"), P("tensor"), P()),
        out_specs=P("tensor", None),
        check_vma=False,
    )
```
